32 devices in a mesh: term: 16 (over z, x, core), sector: 2 (over y).
Axes of the slice: x: 2, y: 2, z: 4, core: 2. Of those that a mesh axis runs over, the one named last changes fastest.
Arguments:
- wavefunction: bfloat16 [4, 512, 512], P('sector'), may hold values from -6 to 6
- left_operators: bfloat16 [256, 512, 512], P(('term', 'sector')), may hold values from -0.25 to 0.25
- right_operators: bfloat16 [256, 512, 512], P(('term', 'sector')), may hold values from -0.25 to 0.25
- source_sector: int32 [256], P(('term', 'sector')), may hold values from 0 to 3
- target_sector: int32 [256], P(('term', 'sector')), may hold values from 0 to 3
- live_terms: int32 [32], P(('term', 'sector')), may hold values from 1 to 8, as said below
- sector_rows: int32 [4], replicated, may hold values from 1 to 512, as said below
Outputs:
- sigma_blocks: float32 [4, 512, 512], P('sector', 'term')
The draws below stay inside these ranges and needn't reach their ends.
Inputs may be any that keep to these rules, and one draw needn't show every extreme that they name: Term group g = term index * 2 + sector index holds the term slots g * 8 to (g + 1) * 8 - 1; its live slots are the first live_terms[g]; some group has exactly 8. `sector_rows`: some sector uses exactly 512 rows.
All inputs are finite; a program needn't handle non-finite values.
Results may differ from the reference program's by a relative error of at most 0.0029.
Values may be sent and summed in bfloat16 or wider, within the bound.
A program may use at most 128 MiB of HBM per device.

```python
import jax
import jax.numpy as jnp
from jax import lax

R = 512
C = 512
TERM_DEV = 8
NSEC = 4
TERMS = 256
GROUPS = 32


def draw_live_terms(key, part):
    first = jax.random.fold_in(key, 11)
    second = jax.random.fold_in(key, 12)
    third = jax.random.fold_in(key, 13)
    small = jax.random.randint(first, (GROUPS,), 1, 3)
    heavy = jax.random.randint(second, (GROUPS,), 0, 16) == 0
    chosen = jax.random.randint(third, (), 0, GROUPS)
    heavy = heavy | (jnp.arange(GROUPS, dtype=jnp.int32) == chosen)
    return jnp.where(heavy, TERM_DEV, small).astype(jnp.int32)


def draw_sector_rows(key, part):
    first = jax.random.fold_in(key, 21)
    second = jax.random.fold_in(key, 22)
    third = jax.random.fold_in(key, 23)
    fourth = jax.random.fold_in(key, 24)
    fifth = jax.random.fold_in(key, 25)
    sizes_one = jax.random.randint(first, (NSEC,), 1, R + 1)
    sizes_two = jax.random.randint(second, (NSEC,), 1, R + 1)
    sizes = jnp.minimum(sizes_one, sizes_two)
    chosen = jax.random.randint(third, (), 0, NSEC)
    offset = jax.random.randint(fourth, (), 1, NSEC)
    partner = (chosen + offset) % NSEC
    partner_rows = jax.random.randint(fifth, (), R // 2, R)
    sector_ids = jnp.arange(NSEC, dtype=jnp.int32)
    sizes = jnp.where(sector_ids == partner, partner_rows, sizes)
    sizes = jnp.where(sector_ids == chosen, R, sizes)
    return sizes.astype(jnp.int32)


def set_ends(values, stream_key, smallest, high):
    longest = values.shape.index(max(values.shape))
    spots = []
    for shift in (0, 1):
        where = [jax.random.randint(jax.random.fold_in(stream_key, axis), (), 0, length) for axis, length in enumerate(values.shape)]
        where[longest] = (where[longest] + shift) % values.shape[longest]
        spots.append(tuple(where))
    return values.at[spots[0]].set(smallest).at[spots[1]].set(high)


def block_levels(stream_key, dims, pieces, low, largest):
    factor_of, own = 1.0, jax.random.fold_in(stream_key, 6)
    for position, blocks in pieces:
        steps = jnp.exp(jax.random.uniform(jax.random.fold_in(own, position), (blocks,), jnp.float32, low / len(pieces), largest / len(pieces)))
        factor_of = factor_of * jnp.repeat(steps, dims[position] // blocks).reshape([-1 if axis == position else 1 for axis in range(len(dims))])
    return factor_of


def normal_values(own_key, extent, deviation, reach, pieces=(), kind=jnp.bfloat16):
    result = jax.random.normal(own_key, extent, jnp.float32) * deviation
    if len(pieces) > 0:
        result = block_levels(own_key, extent, pieces, -0.22, 0.18) * result
    return jnp.clip(result, min=-reach, max=reach).astype(kind)


def setup_inputs(seed: int = 0) -> dict:
    key_of = jax.random.split(jax.random.key(seed), 8)
    wavefunction = normal_values(key_of[0], (NSEC, R, C), 1.0, 6.0, ((0, 2),))
    left_operators = normal_values(key_of[1], (TERMS, R, R), R ** -0.5, 0.25, ((0, 32),))
    right_operators = normal_values(key_of[2], (TERMS, C, C), C ** -0.5, 0.25, ((0, 32),))
    source_sector = set_ends(jax.random.randint(key_of[3], (TERMS,), 0, NSEC), jax.random.fold_in(key_of[3], 1), 0, NSEC - 1).astype(jnp.int32)
    target_sector = set_ends(jax.random.randint(key_of[4], (TERMS,), 0, NSEC), jax.random.fold_in(key_of[4], 1), 0, NSEC - 1).astype(jnp.int32)
    live_terms = draw_live_terms(jax.random.fold_in(key_of[7], 71), 0)
    sector_rows = draw_sector_rows(jax.random.fold_in(key_of[7], 71), 0)
    return dict(wavefunction=wavefunction, left_operators=left_operators, right_operators=right_operators, source_sector=source_sector, target_sector=target_sector, live_terms=live_terms, sector_rows=sector_rows)


def reference(wavefunction, left_operators, right_operators, source_sector, target_sector, live_terms, sector_rows):
    row_ids = jnp.arange(R, dtype=jnp.int32)
    slot_ids = jnp.arange(TERMS, dtype=jnp.int32)
    live_mask = (slot_ids % TERM_DEV) < live_terms[slot_ids // TERM_DEV]
    sigma = jnp.zeros((NSEC, R, C), jnp.float32)

    def apply_term(slot, partial_value):
        def contribute(partial_value):
            source_index = source_sector[slot].astype(jnp.int32)
            target_index = target_sector[slot].astype(jnp.int32)
            source = lax.dynamic_index_in_dim(wavefunction, source_index, 0, keepdims=False)
            keep_rows = (row_ids < sector_rows[source_index])[:, None]
            source = jnp.where(keep_rows, source, jnp.zeros_like(source))
            left_half = jnp.dot(left_operators[slot], source, preferred_element_type=jnp.float32).astype(jnp.bfloat16)
            product = lax.dot_general(left_half, right_operators[slot], (((1,), (1,)), ((), ())), preferred_element_type=jnp.float32)
            current = lax.dynamic_index_in_dim(partial_value, target_index, 0, keepdims=True)
            return lax.dynamic_update_index_in_dim(partial_value, current + product[None], target_index, 0)

        return lax.cond(live_mask[slot], contribute, lambda kept: kept, partial_value)

    sigma = lax.fori_loop(0, TERMS, apply_term, sigma)
    used = row_ids[None, :, None] < sector_rows[:, None, None]
    return jnp.where(used, sigma, jnp.zeros_like(sigma))
```

```python
import functools

import jax
import jax.numpy as jnp
from jax import lax
from jax.experimental import pallas as pl
from jax.experimental.pallas import tpu as pltpu
from jax.sharding import PartitionSpec as P

BF16 = jnp.bfloat16
F32 = jnp.float32


def kernel(
    dims,
    wave,
    left,
    right,
    source_ref,
    target_ref,
    live_ref,
    rows_ref,
    out,
    wv,
    lbuf,
    rbuf,
    prod,
    snd_a0,
    snd_b0,
    rcv_a0,
    rcv_b0,
    acc_a,
    acc_b,
    snd_a1,
    rcv_a1,
    snd_b1,
    rcv_b1,
    snd_a2,
    rcv_a2,
    snd_b2,
    rcv_b2,
    snd_a3,
    rcv_a3,
    snd_b3,
    rcv_b3,
    load_sem,
    g_send,
    g_recv,
    f_send,
    f_recv,
    s0,
    r0,
    sx,
    rx,
    sy_b,
    ry_b,
    sy_a,
    ry_a,
    sz_a,
    rz_a,
    sz_b,
    rz_b,
):
    Z, X, S, K, B, C = dims
    H = C // 2
    slots = left.shape[0]
    term = lax.axis_index("term")
    ym = lax.axis_index("sector")
    cm = lax.rem(term, 2)
    xm = lax.rem(term // 2, X)
    zm = term // (2 * X)
    co = 1 - cm
    xo = 1 - xm

    def dev(z, x, c, y):
        return ((z * X + x) * 2 + c, y)

    core_peer = dev(zm, xm, co, ym)
    x_peer = dev(zm, xo, cm, ym)

    def y_peer(d):
        return dev(zm, xm, cm, lax.rem(ym + d, S))

    def z_peer(d):
        return dev(lax.rem(zm + d, Z), xm, cm, ym)

    def remote(src, dst, ssem, rsem, peer):
        return pltpu.make_async_remote_copy(
            src_ref=src,
            dst_ref=dst,
            send_sem=ssem,
            recv_sem=rsem,
            device_id=peer,
            device_id_type=pl.DeviceIdType.MESH,
        )

    mine = pl.ds(ym * K, K)
    own_loads = []
    for n, half in enumerate((cm, co)):
        cols = pl.ds(pl.multiple_of(half * H, 128), H)
        own_loads.append(pltpu.make_async_copy(wave.at[:, :, cols], wv.at[half, mine], load_sem.at[n]))
    l_loads = [
        pltpu.make_async_copy(left.at[:, :, c], lbuf.at[c], load_sem.at[2 + c]) for c in range(2)
    ]
    r_load = pltpu.make_async_copy(right, rbuf, load_sem.at[4])
    for cp in own_loads:
        cp.start()
    for cp in l_loads:
        cp.start()
    r_load.start()

    barrier = pltpu.get_barrier_semaphore()
    peers = [core_peer, x_peer]
    peers += [y_peer(d) for d in range(1, S)]
    peers += [z_peer(d) for d in range(1, Z)]
    for peer in peers:
        pl.semaphore_signal(barrier, inc=1, device_id=peer, device_id_type=pl.DeviceIdType.MESH)
    pl.semaphore_wait(barrier, len(peers))

    own_loads[0].wait()
    gathers = []
    for d in range(1, S):
        cp = remote(wv.at[cm, mine], wv.at[cm, mine], g_send.at[d - 1], g_recv.at[d - 1], y_peer(d))
        cp.start()
        gathers.append(cp)
    own_loads[1].wait()
    forwards = []
    for d in range(1, S):
        theirs = pl.ds(lax.rem(ym + S - d, S) * K, K)
        remote(
            wv.at[cm, theirs], wv.at[cm, theirs], g_send.at[d - 1], g_recv.at[d - 1], y_peer(d)
        ).wait_recv()
        cp = remote(
            wv.at[cm, theirs], wv.at[cm, theirs], f_send.at[d - 1], f_recv.at[d - 1], core_peer
        )
        cp.start()
        forwards.append(cp)
    for cp in l_loads:
        cp.wait()
    r_load.wait()
    for d in range(1, S):
        theirs = pl.ds(lax.rem(ym + S - d, S) * K, K)
        remote(
            wv.at[co, theirs], wv.at[co, theirs], f_send.at[d - 1], f_recv.at[d - 1], core_peer
        ).wait_recv()

    depth_ids = lax.broadcasted_iota(jnp.int32, (1, wv.shape[2]), 1)

    def products(c):
        @pl.loop(0, slots)
        def _(t):
            source = source_ref[t]
            limit = jnp.where(t < live_ref[0], rows_ref[source], 0)
            keep = jnp.where(depth_ids < limit, 1.0, 0.0).astype(BF16)
            lmat = lbuf[c, t].reshape(Z * X * B, -1) * keep
            total = None
            for h in range(2):
                half = jnp.dot(lmat, wv[h, source], preferred_element_type=F32).astype(BF16)
                part = lax.dot_general(
                    half,
                    rbuf[t, :, h * H : (h + 1) * H],
                    (((1,), (1,)), ((), ())),
                    preferred_element_type=F32,
                )
                total = part if total is None else total + part
            prod[t] = total

    def sums(store):
        @pl.loop(0, S * K * Z * X)
        def _(n):
            s = n // (Z * X)
            zx = n % (Z * X)
            y, k = s // K, s % K
            z, x = zx // X, zx % X
            rows = pl.ds(pl.multiple_of(zx * B, B), B)
            total = jnp.zeros((B, C), F32)
            for t in range(slots):
                weight = jnp.where(target_ref[t] == s, 1.0, 0.0)
                total = total + prod[t, rows, :] * weight
            store(y, k, z, x, total)

    def store_send(y, k, z, x, total):
        snd_a0[x, y, z, k] = total[:, :H].astype(BF16)
        snd_b0[y, x, z, k] = total[:, H:].astype(BF16)

    def store_own(y, k, z, x, total):
        acc_a[x, y, z, k] = total[:, :H]
        acc_b[y, x, z, k] = total[:, H:]

    products(co)
    sums(store_send)
    a0 = remote(snd_a0, rcv_a0, s0.at[0], r0.at[0], core_peer)
    b0 = remote(snd_b0, rcv_b0, s0.at[1], r0.at[1], core_peer)
    a0.start()
    b0.start()
    products(cm)
    sums(store_own)

    a0.wait_recv()
    snd_a1[...] = (acc_a[xo] + rcv_a0[xo].astype(F32)).astype(BF16)
    a1 = remote(snd_a1, rcv_a1, sx.at[0], rx.at[0], x_peer)
    a1.start()
    b0.wait_recv()
    b1 = []
    for d in range(1, S):
        yo = lax.rem(ym + d, S)
        snd_b1[d - 1] = (acc_b[yo] + rcv_b0[yo].astype(F32)).astype(BF16)
        cp = remote(snd_b1.at[d - 1], rcv_b1.at[d - 1], sy_b.at[d - 1], ry_b.at[d - 1], y_peer(d))
        cp.start()
        b1.append(cp)

    a1.wait_recv()
    a2 = []
    for d in range(1, S):
        yo = lax.rem(ym + d, S)
        snd_a2[d - 1] = (
            acc_a[xm, yo] + rcv_a0[xm, yo].astype(F32) + rcv_a1[yo].astype(F32)
        ).astype(BF16)
        cp = remote(snd_a2.at[d - 1], rcv_a2.at[d - 1], sy_a.at[d - 1], ry_a.at[d - 1], y_peer(d))
        cp.start()
        a2.append(cp)
    for cp in b1:
        cp.wait_recv()

    def b_sum(x):
        total = acc_b[ym, x] + rcv_b0[ym, x].astype(F32)
        for d in range(1, S):
            total = total + rcv_b1[d - 1, x].astype(F32)
        return total

    snd_b2[...] = b_sum(xo).astype(BF16)
    b2 = remote(snd_b2, rcv_b2, sx.at[1], rx.at[1], x_peer)
    b2.start()

    def a_last(z):
        total = acc_a[xm, ym, z] + rcv_a0[xm, ym, z].astype(F32) + rcv_a1[ym, z].astype(F32)
        for d in range(1, S):
            total = total + rcv_a2[d - 1, z].astype(F32)
        return total

    def b_last(z):
        total = acc_b[ym, xm, z] + rcv_b0[ym, xm, z].astype(F32)
        for d in range(1, S):
            total = total + rcv_b1[d - 1, xm, z].astype(F32)
        return total + rcv_b2[z].astype(F32)

    for cp in a2:
        cp.wait_recv()
    a3, b3 = [], []
    for d in range(1, Z):
        snd_a3[d - 1] = a_last(lax.rem(zm + d, Z)).astype(BF16)
        cp = remote(snd_a3.at[d - 1], rcv_a3.at[d - 1], sz_a.at[d - 1], rz_a.at[d - 1], z_peer(d))
        cp.start()
        a3.append(cp)
    b2.wait_recv()
    for d in range(1, Z):
        snd_b3[d - 1] = b_last(lax.rem(zm + d, Z)).astype(BF16)
        cp = remote(snd_b3.at[d - 1], rcv_b3.at[d - 1], sz_b.at[d - 1], rz_b.at[d - 1], z_peer(d))
        cp.start()
        b3.append(cp)

    ids = term * B + lax.broadcasted_iota(jnp.int32, (B, H), 0)
    for own, copies, received, h in ((a_last, a3, rcv_a3, 0), (b_last, b3, rcv_b3, 1)):
        total = own(zm)
        for d, cp in enumerate(copies):
            cp.wait_recv()
            total = total + received[d].astype(F32)
        for k in range(K):
            used = ids < rows_ref[ym * K + k]
            out[k, :, h * H : (h + 1) * H] = jnp.where(used, total[k], 0.0)

    for cp in gathers + forwards + [a0, b0, a1, b2] + b1 + a2 + a3 + b3:
        cp.wait_send()


def local(mesh_sizes, wave, left, right, source, target, live, sector_rows):
    T, S = mesh_sizes
    X = 2
    Z = T // (2 * X)
    K, R, C = wave.shape
    B = R // T
    H = C // 2
    slots = left.shape[0]
    dims = (Z, X, S, K, B, C)
    left = left.reshape(slots, Z * X, 2, B, R)
    vm = pltpu.VMEM
    dma = pltpu.SemaphoreType.DMA
    full_a = (X, S, Z, K, B, H)
    full_b = (S, X, Z, K, B, H)
    scratch = [
        vm((2, S * K, R, H), BF16),
        vm((2, slots, Z * X, B, R), BF16),
        vm((slots, C, C), BF16),
        vm((slots, R // 2, C), F32),
        vm(full_a, BF16),
        vm(full_b, BF16),
        vm(full_a, BF16),
        vm(full_b, BF16),
        vm(full_a, F32),
        vm(full_b, F32),
        vm(full_a[1:], BF16),
        vm(full_a[1:], BF16),
        vm((S - 1,) + full_b[1:], BF16),
        vm((S - 1,) + full_b[1:], BF16),
        vm((S - 1, Z, K, B, H), BF16),
        vm((S - 1, Z, K, B, H), BF16),
        vm((Z, K, B, H), BF16),
        vm((Z, K, B, H), BF16),
        vm((Z - 1, K, B, H), BF16),
        vm((Z - 1, K, B, H), BF16),
        vm((Z - 1, K, B, H), BF16),
        vm((Z - 1, K, B, H), BF16),
        dma((5,)),
        dma((S - 1,)),
        dma((S - 1,)),
        dma((S - 1,)),
        dma((S - 1,)),
        dma((2,)),
        dma((2,)),
        dma((2,)),
        dma((2,)),
        dma((S - 1,)),
        dma((S - 1,)),
        dma((S - 1,)),
        dma((S - 1,)),
        dma((Z - 1,)),
        dma((Z - 1,)),
        dma((Z - 1,)),
        dma((Z - 1,)),
    ]
    any_spec = pl.BlockSpec(memory_space=pl.ANY)
    smem = pl.BlockSpec(memory_space=pltpu.SMEM)
    return pl.pallas_call(
        functools.partial(kernel, dims),
        out_shape=jax.ShapeDtypeStruct((K, B, C), F32),
        in_specs=[any_spec] * 3 + [smem] * 4,
        out_specs=pl.BlockSpec(memory_space=pltpu.VMEM),
        scratch_shapes=scratch,
        compiler_params=pltpu.CompilerParams(
            collective_id=0, has_side_effects=True, vmem_limit_bytes=60 * 1024 * 1024
        ),
    )(wave, left, right, source, target, live, sector_rows)


def solution(mesh):
    in_specs = (
        P("sector", None, None),
        P(("term", "sector"), None, None),
        P(("term", "sector"), None, None),
        P(("term", "sector")),
        P(("term", "sector")),
        P(("term", "sector")),
        P(),
    )
    out_specs = P("sector", "term", None)
    sizes = (mesh.shape["term"], mesh.shape["sector"])
    return jax.shard_map(
        functools.partial(local, sizes),
        mesh=mesh,
        in_specs=in_specs,
        out_specs=out_specs,
        check_vma=False,
    )
```

```python
import functools

import jax
import jax.numpy as jnp
from jax import lax
from jax.experimental import pallas as pl
from jax.experimental.pallas import tpu as pltpu
from jax.sharding import PartitionSpec as P

BF16 = jnp.bfloat16
F32 = jnp.float32


def kernel(
    dims,
    wave,
    left,
    right,
    source_ref,
    target_ref,
    live_ref,
    rows_ref,
    out,
    near,
    far,
    lbuf,
    rbuf,
    prod,
    snd_a0,
    snd_b0,
    rcv_a0,
    rcv_b0,
    acc_a,
    acc_b,
    snd_a1,
    rcv_a1,
    snd_b1,
    rcv_b1,
    snd_a2,
    rcv_a2,
    snd_b2,
    rcv_b2,
    snd_a3,
    rcv_a3,
    snd_b3,
    rcv_b3,
    order,
    joins,
    load_sem,
    g_send,
    g_recv,
    h_send,
    h_recv,
    f_send,
    f_recv,
    s0,
    r0,
    sx,
    rx,
    sy_b,
    ry_b,
    sy_a,
    ry_a,
    sz,
    rz,
):
    Z, X, S, K, B, C = dims
    H, Q = C // 2, C // 4
    R = wave.shape[1]
    slots = left.shape[0]
    term = lax.axis_index("term")
    ym = lax.axis_index("sector")
    cm = lax.rem(term, 2)
    xm = lax.rem(term // 2, X)
    zm = term // (2 * X)
    co = 1 - cm
    xo = 1 - xm

    def dev(z, x, c, y):
        return ((z * X + x) * 2 + c, y)

    core_peer = dev(zm, xm, co, ym)
    x_peer = dev(zm, xo, cm, ym)

    def y_peer(d):
        return dev(zm, xm, cm, lax.rem(ym + d, S))

    def z_peer(d):
        return dev(lax.rem(zm + d, Z), xm, cm, ym)

    def remote(src, dst, ssem, rsem, peer):
        return pltpu.make_async_remote_copy(
            src_ref=src,
            dst_ref=dst,
            send_sem=ssem,
            recv_sem=rsem,
            device_id=peer,
            device_id_type=pl.DeviceIdType.MESH,
        )

    mine = pl.ds(ym * K, K)
    own_loads = []
    for n, (half, held) in enumerate(((xm, near), (xo, far))):
        cols = pl.ds(pl.multiple_of(half * H, 128), H)
        own_loads.append(
            pltpu.make_async_copy(wave.at[:, :, cols], held.at[mine], load_sem.at[n])
        )
    l_loads = [
        pltpu.make_async_copy(left.at[:, :, c], lbuf.at[:, c], load_sem.at[2 + c]) for c in range(2)
    ]
    l_loads += [
        pltpu.make_async_copy(right.at[:, :, h * H : (h + 1) * H], rbuf.at[h], load_sem.at[4 + h])
        for h in range(2)
    ]
    for cp in own_loads:
        cp.start()
    for cp in l_loads:
        cp.start()

    barrier = pltpu.get_barrier_semaphore()
    peers = [core_peer, x_peer]
    peers += [y_peer(d) for d in range(1, S)]
    peers += [z_peer(d) for d in range(1, Z)]
    for peer in peers:
        pl.semaphore_signal(barrier, inc=1, device_id=peer, device_id_type=pl.DeviceIdType.MESH)
    pl.semaphore_wait(barrier, len(peers))

    def part(held, d, j, c):
        sector = lax.rem(ym + S - d, S) * K + j // 4
        rows = pl.ds((j % 4) * (R // 4), R // 4)
        return held.at[sector, rows, pl.ds(pl.multiple_of(c * Q, 128), Q)]

    pieces = [(d, j) for j in range(4 * K) for d in range(1, S)]

    def y_copy(d, j, source):
        ref = part(near, source, j, cm)
        return remote(ref, ref, g_send.at[d - 1, j], g_recv.at[d - 1, j], y_peer(d))

    def x_copy(d, j):
        ref = part(near, d, j, cm)
        return remote(ref, part(far, d, j, cm), h_send.at[d - 1, j], h_recv.at[d - 1, j], x_peer)

    def core_copy(d, j, held, c, n):
        ref = part(held, d, j, c)
        return remote(ref, ref, f_send.at[n, d - 1, j], f_recv.at[n, d - 1, j], core_peer)

    sent = []
    own_loads[0].wait()
    for d, j in pieces:
        cp = y_copy(d, j, 0)
        cp.start()
        sent.append(cp)
    own_loads[1].wait()

    targets = [target_ref[t] for t in range(slots)]
    ranks = []
    for t in range(slots):
        rank = jnp.int32(0)
        for u in range(slots):
            ahead = targets[u] <= targets[t] if u < t else targets[u] < targets[t]
            if u != t:
                rank = rank + jnp.where(ahead, 1, 0)
        ranks.append(rank)
    before = jnp.int32(-1)
    for n in range(slots):
        slot, target = jnp.int32(0), jnp.int32(0)
        for t in range(slots):
            slot = jnp.where(ranks[t] == n, t, slot)
            target = jnp.where(ranks[t] == n, targets[t], target)
        order[n] = slot
        joins[n] = jnp.where(target == before, 1.0, 0.0)
        before = target
    prod[0] = jnp.zeros(prod.shape[1:], F32)
    for d, j in pieces:
        y_copy(d, j, d).wait_recv()
        for cp in (x_copy(d, j), core_copy(d, j, near, cm, 0)):
            cp.start()
            sent.append(cp)
    for cp in l_loads:
        cp.wait()
    for d, j in pieces:
        core_copy(d, j, near, co, 0).wait_recv()

    depth_ids = lax.broadcasted_iota(jnp.int32, (1, R), 1)
    chunk = 4 if slots % 8 == 0 else 1

    def products(held, h, first, begin, end):
        def one(n):
            t = order[n]
            source = source_ref[t]
            limit = jnp.where(t < live_ref[0], rows_ref[source], 0)
            keep = jnp.where(depth_ids < limit, 1.0, 0.0).astype(BF16)
            lmat = lbuf[t].reshape(R, R) * keep
            half = jnp.dot(lmat, held[source], preferred_element_type=F32).astype(BF16)
            return lax.dot_general(
                half,
                rbuf[h, t],
                (((1,), (1,)), ((), ())),
                preferred_element_type=F32,
            )

        @pl.loop(begin // chunk, end // chunk)
        def _(m):
            for u in range(chunk):
                n = m * chunk + u
                total = one(n)
                if not first:
                    total = total + prod[n + 1] + prod[n] * joins[n]
                prod[n + 1] = total

    def sums(c, store):
        @pl.loop(0, S * K * Z * X)
        def _(m):
            s = m // (Z * X)
            zx = m % (Z * X)
            y, k = s // K, s % K
            z, x = zx // X, zx % X
            rows = pl.ds(pl.multiple_of((c * Z * X + zx) * B, B), B)
            upto = jnp.int32(0)
            below = jnp.int32(0)
            for t in range(slots):
                upto = upto + jnp.where(target_ref[t] <= s, 1, 0)
                below = below + jnp.where(target_ref[t] < s, 1, 0)
            store(y, k, z, x, prod[upto, rows, :] * jnp.where(upto > below, 1.0, 0.0))

    def store_send(y, k, z, x, total):
        for i in range(2):
            snd_a0[i, x, y, z, k] = total[:, 2 * i * Q : (2 * i + 1) * Q].astype(BF16)
            snd_b0[i, y, x, z, k] = total[:, (2 * i + 1) * Q : (2 * i + 2) * Q].astype(BF16)

    def store_own(y, k, z, x, total):
        for i in range(2):
            acc_a[i, x, y, z, k] = total[:, 2 * i * Q : (2 * i + 1) * Q]
            acc_b[i, y, x, z, k] = total[:, (2 * i + 1) * Q : (2 * i + 2) * Q]

    products(near, xm, True, 0, slots // 2)
    for d, j in pieces:
        x_copy(d, j).wait_recv()
        cp = core_copy(d, j, far, cm, 1)
        cp.start()
        sent.append(cp)
    products(near, xm, True, slots // 2, slots)
    for d, j in pieces:
        core_copy(d, j, far, co, 1).wait_recv()
    products(far, xo, False, 0, slots)
    sums(co, store_send)
    a0, b0 = [], []
    for i in range(2):
        a0.append(remote(snd_a0.at[i], rcv_a0.at[i], s0.at[0, i], r0.at[0, i], core_peer))
        b0.append(remote(snd_b0.at[i], rcv_b0.at[i], s0.at[1, i], r0.at[1, i], core_peer))
        a0[i].start()
        b0[i].start()
    sums(cm, store_own)

    a1, b1 = [], [[], []]
    for i in range(2):
        a0[i].wait_recv()
        snd_a1[i] = (acc_a[i, xo] + rcv_a0[i, xo].astype(F32)).astype(BF16)
        cp = remote(snd_a1.at[i], rcv_a1.at[i], sx.at[0, i], rx.at[0, i], x_peer)
        cp.start()
        a1.append(cp)
        b0[i].wait_recv()
        for d in range(1, S):
            yo = lax.rem(ym + d, S)
            snd_b1[i, d - 1] = (acc_b[i, yo] + rcv_b0[i, yo].astype(F32)).astype(BF16)
            cp = remote(
                snd_b1.at[i, d - 1],
                rcv_b1.at[i, d - 1],
                sy_b.at[i, d - 1],
                ry_b.at[i, d - 1],
                y_peer(d),
            )
            cp.start()
            b1[i].append(cp)

    def b_sum(i, x):
        total = acc_b[i, ym, x] + rcv_b0[i, ym, x].astype(F32)
        for d in range(1, S):
            total = total + rcv_b1[i, d - 1, x].astype(F32)
        return total

    a2, b2 = [[], []], []
    for i in range(2):
        a1[i].wait_recv()
        for d in range(1, S):
            yo = lax.rem(ym + d, S)
            snd_a2[i, d - 1] = (
                acc_a[i, xm, yo] + rcv_a0[i, xm, yo].astype(F32) + rcv_a1[i, yo].astype(F32)
            ).astype(BF16)
            cp = remote(
                snd_a2.at[i, d - 1],
                rcv_a2.at[i, d - 1],
                sy_a.at[i, d - 1],
                ry_a.at[i, d - 1],
                y_peer(d),
            )
            cp.start()
            a2[i].append(cp)
        for cp in b1[i]:
            cp.wait_recv()
        snd_b2[i] = b_sum(i, xo).astype(BF16)
        cp = remote(snd_b2.at[i], rcv_b2.at[i], sx.at[1, i], rx.at[1, i], x_peer)
        cp.start()
        b2.append(cp)

    def a_last(i, z):
        total = (
            acc_a[i, xm, ym, z]
            + rcv_a0[i, xm, ym, z].astype(F32)
            + rcv_a1[i, ym, z].astype(F32)
        )
        for d in range(1, S):
            total = total + rcv_a2[i, d - 1, z].astype(F32)
        return total

    def b_last(i, z):
        total = acc_b[i, ym, xm, z] + rcv_b0[i, ym, xm, z].astype(F32)
        for d in range(1, S):
            total = total + rcv_b1[i, d - 1, xm, z].astype(F32)
        return total + rcv_b2[i, z].astype(F32)

    z3 = []
    far_first = sorted(range(1, Z), key=lambda d: -min(d, Z - d))
    for i in range(2):
        for cp in a2[i]:
            cp.wait_recv()
        for n, own, snd, rcv in ((0, a_last, snd_a3, rcv_a3), (1, b_last, snd_b3, rcv_b3)):
            if n == 1:
                b2[i].wait_recv()
            copies = {}
            for d in far_first:
                snd[i, d - 1] = own(i, lax.rem(zm + d, Z)).astype(BF16)
                cp = remote(
                    snd.at[i, d - 1],
                    rcv.at[i, d - 1],
                    sz.at[n, i, d - 1],
                    rz.at[n, i, d - 1],
                    z_peer(d),
                )
                cp.start()
                copies[d] = cp
            z3.append((i, n, own, rcv, copies))

    ids = term * B + lax.broadcasted_iota(jnp.int32, (B, Q), 0)
    for i, n, own, rcv, copies in z3:
        total = own(i, zm)
        for d in range(1, Z):
            copies[d].wait_recv()
            total = total + rcv[i, d - 1].astype(F32)
            sent.append(copies[d])
        col = (2 * i + n) * Q
        for k in range(K):
            used = ids < rows_ref[ym * K + k]
            out[k, :, col : col + Q] = jnp.where(used, total[k], 0.0)

    sent += a0 + b0 + a1 + b2 + b1[0] + b1[1] + a2[0] + a2[1]
    for cp in sent:
        cp.wait_send()


def local(mesh_sizes, wave, left, right, source, target, live, sector_rows):
    T, S = mesh_sizes
    X = 2
    Z = T // (2 * X)
    K, R, C = wave.shape
    B = R // T
    H, Q = C // 2, C // 4
    slots = left.shape[0]
    dims = (Z, X, S, K, B, C)
    left = left.reshape(slots, Z * X, 2, B, R)
    vm = pltpu.VMEM
    dma = pltpu.SemaphoreType.DMA
    full_a = (2, X, S, Z, K, B, Q)
    full_b = (2, S, X, Z, K, B, Q)
    after_x = (2, S, Z, K, B, Q)
    after_y = (2, S - 1, X, Z, K, B, Q)
    both = (2, Z, K, B, Q)
    after_y2 = (2, S - 1, Z, K, B, Q)
    last = (2, Z - 1, K, B, Q)
    scratch = [
        vm((S * K, R, H), BF16),
        vm((S * K, R, H), BF16),
        vm((slots, 2, Z * X, B, R), BF16),
        vm((2, slots, C, H), BF16),
        vm((slots + 1, R, C), F32),
        vm(full_a, BF16),
        vm(full_b, BF16),
        vm(full_a, BF16),
        vm(full_b, BF16),
        vm(full_a, F32),
        vm(full_b, F32),
        vm(after_x, BF16),
        vm(after_x, BF16),
        vm(after_y, BF16),
        vm(after_y, BF16),
        vm(after_y2, BF16),
        vm(after_y2, BF16),
        vm(both, BF16),
        vm(both, BF16),
        vm(last, BF16),
        vm(last, BF16),
        vm(last, BF16),
        vm(last, BF16),
        pltpu.SMEM((slots,), jnp.int32),
        pltpu.SMEM((slots,), F32),
        dma((6,)),
        dma((S - 1, 4 * K)),
        dma((S - 1, 4 * K)),
        dma((S - 1, 4 * K)),
        dma((S - 1, 4 * K)),
        dma((2, S - 1, 4 * K)),
        dma((2, S - 1, 4 * K)),
        dma((2, 2)),
        dma((2, 2)),
        dma((2, 2)),
        dma((2, 2)),
        dma((2, S - 1)),
        dma((2, S - 1)),
        dma((2, S - 1)),
        dma((2, S - 1)),
        dma((2, 2, Z - 1)),
        dma((2, 2, Z - 1)),
    ]
    any_spec = pl.BlockSpec(memory_space=pl.ANY)
    smem = pl.BlockSpec(memory_space=pltpu.SMEM)
    return pl.pallas_call(
        functools.partial(kernel, dims),
        out_shape=jax.ShapeDtypeStruct((K, B, C), F32),
        in_specs=[any_spec] * 3 + [smem] * 4,
        out_specs=pl.BlockSpec(memory_space=pltpu.VMEM),
        scratch_shapes=scratch,
        compiler_params=pltpu.CompilerParams(
            collective_id=0, has_side_effects=True, vmem_limit_bytes=60 * 1024 * 1024
        ),
    )(wave, left, right, source, target, live, sector_rows)


def solution(mesh):
    in_specs = (
        P("sector", None, None),
        P(("term", "sector"), None, None),
        P(("term", "sector"), None, None),
        P(("term", "sector")),
        P(("term", "sector")),
        P(("term", "sector")),
        P(),
    )
    out_specs = P("sector", "term", None)
    sizes = (mesh.shape["term"], mesh.shape["sector"])
    return jax.shard_map(
        functools.partial(local, sizes),
        mesh=mesh,
        in_specs=in_specs,
        out_specs=out_specs,
        check_vma=False,
    )
```
